32 devices in a mesh: tile: 8 (over z, y), col: 4 (over x, core).
Axes of the slice: x: 2, y: 2, z: 4, core: 2. Of those that a mesh axis runs over, the one named last changes fastest.
Arguments:
- latent: bfloat16 [8, 17, 4, 16, 256], P('tile', None, None, 'col'), may hold values from -20 to 20
- intersections: int32 [8], P('tile'), may hold values from 0 to 4, as said below
- norm_gain_one: float32 [256], replicated, may hold values from 0.5 to 1.5
- norm_shift_one: float32 [256], replicated, may hold values from -3 to 3
- weight_one: bfloat16 [3, 3, 3, 256, 256], P(None, None, None, 'col'), may hold values from -0.078125 to 0.078125
- norm_gain_two: float32 [256], replicated, may hold values from 0.5 to 1.5
- norm_shift_two: float32 [256], replicated, may hold values from -3 to 3
- weight_two: bfloat16 [3, 3, 3, 256, 256], P(None, None, None, 'col'), may hold values from -0.078125 to 0.078125
- conv_bias: float32 [256], replicated, may hold values from -1.8 to 1.8
Outputs:
- blended: bfloat16 [8, 17, 4, 16, 256], P('tile', None, None, 'col')
The draws below stay inside these ranges and needn't reach their ends.
Inputs may be any that keep to these rules, and one draw needn't show every extreme that they name: intersections[0] is 0 and every other entry is 1 to 4; some entry equals 4.
All inputs are finite; a program needn't handle non-finite values.
Results may differ from the reference program's by a relative error of at most 0.0055.
Values may be sent and summed in bfloat16 or wider, within the bound.
A program may use at most 64 MiB of HBM per device.

```python
import jax
import jax.numpy as jnp
from jax import lax

C = 256
GROUPS = 32
FT = 17
OVMAX = 4
H = 4
TILES = 8
W = 16


def draw_latent(key, part):
    shape = (TILES, FT, H, W, C)
    column = jnp.arange(W, dtype=jnp.float32) / (W - 1)
    factor = 3.0 ** column
    base = jnp.clip(jax.random.normal(key, shape, jnp.float32), -6.0, 6.0)
    return (base * factor[:, None]).astype(jnp.bfloat16)


def draw_intersections(key, part):
    counts = jax.random.randint(key, (TILES,), 1, OVMAX + 1)
    chosen = jax.random.randint(jax.random.fold_in(key, 7), (), 1, TILES)
    places = jnp.arange(TILES, dtype=jnp.int32)
    counts = jnp.where(places == chosen, OVMAX, counts)
    counts = jnp.where(places == 0, 0, counts)
    return counts.astype(jnp.int32)


def steps_of(rng, shape, shards, least, high):
    factor_of = 1.0
    for dim, blocks in shards:
        draws = jax.random.uniform(jax.random.fold_in(jax.random.fold_in(rng, 6), dim), (blocks,), jnp.float32, least / len(shards), high / len(shards))
        factor_of = factor_of * jnp.repeat(jnp.exp(draws), shape[dim] // blocks).reshape((-1,) + (1,) * (len(shape) - 1 - dim))
    return factor_of


def gaussian(stream_key, dims, scale, bound, cuts=(), kind=jnp.bfloat16):
    factor_of = steps_of(stream_key, dims, cuts, -0.22, 0.18) if cuts else 1.0
    array = jax.random.normal(stream_key, dims, jnp.float32) * scale * factor_of
    return jnp.minimum(jnp.maximum(array, -bound), bound).astype(kind)


def setup_inputs(seed: int = 0) -> dict:
    splits = jax.random.split(jax.random.key(seed), 10)
    return {
        "latent": draw_latent(jax.random.fold_in(splits[9], 71), 0),
        "intersections": draw_intersections(jax.random.fold_in(splits[9], 71), 0),
        "norm_gain_one": jnp.clip(1.0 + 0.1 * jax.random.normal(splits[2], (C,), jnp.float32), 0.5, 1.5),
        "norm_shift_one": gaussian(splits[3], (C,), 0.5, 3.0, (), jnp.float32),
        "weight_one": gaussian(splits[4], (3, 3, 3, C, C), (27 * C) ** -0.5, 0.078125, ((3, 4),)),
        "norm_gain_two": jnp.clip(1.0 + 0.1 * jax.random.normal(splits[5], (C,), jnp.float32), 0.5, 1.5),
        "norm_shift_two": gaussian(splits[6], (C,), 0.5, 3.0, (), jnp.float32),
        "weight_two": gaussian(splits[7], (3, 3, 3, C, C), (27 * C) ** -0.5, 0.078125, ((3, 4),)),
        "conv_bias": gaussian(splits[8], (C,), 0.3, 1.8, (), jnp.float32),
    }


epsilon = 1e-06

def norm_silu(values, gain, shift):
    frames, height, width, channels = values.shape
    per_group = channels // GROUPS
    grouped = values.reshape(frames, height, width, GROUPS, per_group)
    group_mean = lax.optimization_barrier(jnp.mean(grouped, axis=(0, 1, 2, 4)))
    centred = grouped - group_mean[:, None]
    spread = lax.optimization_barrier(jnp.mean(centred * centred, axis=(0, 1, 2, 4)))
    normed = centred * lax.rsqrt(spread + epsilon)[:, None]
    normed = normed.reshape(values.shape) * gain + shift
    return jax.nn.silu(normed).astype(jnp.bfloat16)

def conv_taps(padded, kernel):
    frames = padded.shape[0]
    height = padded.shape[1]
    out_width = padded.shape[2] - 2
    channels = padded.shape[3]
    outputs = kernel.shape[4]
    padded = jnp.pad(padded, ((2, 0), (1, 1), (0, 0), (0, 0)))
    running = jnp.zeros((frames * height * out_width, outputs), jnp.float32)
    for tap_t in range(3):
        for tap_h in range(3):
            for tap_w in range(3):
                window = padded[tap_t:tap_t + frames, tap_h:tap_h + height, tap_w:tap_w + out_width]
                running = running + jnp.dot(window.reshape(-1, channels), kernel[tap_t, tap_h, tap_w], preferred_element_type=jnp.float32)
    return running.reshape(frames, height, out_width, outputs)

def reference(latent, intersections, norm_gain_one, norm_shift_one, weight_one, norm_gain_two, norm_shift_two, weight_two, conv_bias):

    def decode_tile(source):
        latent_full = source.astype(jnp.float32)
        act_one = norm_silu(latent_full, norm_gain_one, norm_shift_one)
        padded = jnp.pad(act_one, ((0, 0), (0, 0), (1, 1), (0, 0)))
        hidden = conv_taps(padded, weight_one).astype(jnp.bfloat16)
        act_two = norm_silu(hidden.astype(jnp.float32), norm_gain_two, norm_shift_two)
        padded = jnp.pad(act_two, ((0, 0), (0, 0), (1, 1), (0, 0)))
        branch = conv_taps(padded, weight_two) + conv_bias
        return (latent_full + branch).astype(jnp.bfloat16)
    decoded = lax.map(decode_tile, latent)
    frames = decoded.shape[1]
    prev_tails = jnp.concatenate([jnp.zeros_like(decoded[:1, :OVMAX]), decoded[:-1, frames - OVMAX:]], axis=0)
    extended = jnp.concatenate([prev_tails, jnp.zeros_like(prev_tails)], axis=1)

    def align(ext_tile, shared):
        return lax.dynamic_slice_in_dim(ext_tile, (OVMAX - shared).astype(jnp.int32), OVMAX, 0)
    aligned = jax.vmap(align)(extended, intersections)
    position = jnp.arange(OVMAX, dtype=jnp.int32)
    own_share = (position[None, :] + 1).astype(jnp.float32) / (intersections[:, None] + 1).astype(jnp.float32)
    own_share = own_share[:, :, None, None, None]
    head = decoded[:, :OVMAX].astype(jnp.float32)
    active = position[None, :, None, None, None] < intersections[:, None, None, None, None]
    mixed = jnp.where(active, own_share * head + (1.0 - own_share) * aligned.astype(jnp.float32), head)
    return jnp.concatenate([mixed.astype(jnp.bfloat16), decoded[:, OVMAX:]], axis=1)
```

```python
import functools

import jax
import jax.numpy as jnp
from jax import lax
from jax.experimental import pallas as pl
from jax.experimental.pallas import tpu as pltpu
from jax.sharding import PartitionSpec as P

GROUPS = 32
OVMAX = 4


epsilon = 1e-06


def extended_2(array, sides, width):
    for axis, dim in sides:
        size, length = (lax.axis_size(axis), array.shape[dim])
        up = [(i, (i + 1) % size) for i in range(size - 1)]
        down = [(j, i) for i, j in up]
        last = lax.slice_in_dim(array, length - width, length, axis=dim)
        first = lax.slice_in_dim(array, 0, width, axis=dim)
        before = lax.ppermute(last, axis, up)
        after = lax.ppermute(first, axis, down)
        array = jnp.concatenate([before, array, after], axis=dim)
    return array


def shifted(block, axis, distance):
    devices = range(lax.axis_size(axis))
    route = [(i - distance, i) for i in devices if i - distance in devices]
    return lax.ppermute(block, axis, route)


def conv_taps(padded, kernel):
    frames = padded.shape[0]
    height = padded.shape[1]
    out_width = padded.shape[2] - 2
    channels = padded.shape[3]
    outputs = kernel.shape[4]
    padded = jnp.pad(padded, ((2, 0), (1, 1), (0, 0), (0, 0)))
    running = jnp.zeros((frames * height * out_width, outputs), jnp.float32)
    for tap_t in range(3):
        for tap_h in range(3):
            for tap_w in range(3):
                window = padded[
                    tap_t : tap_t + frames, tap_h : tap_h + height, tap_w : tap_w + out_width
                ]
                running = running + jnp.dot(
                    window.reshape(-1, channels),
                    kernel[tap_t, tap_h, tap_w],
                    preferred_element_type=jnp.float32,
                )
    return running.reshape(frames, height, out_width, outputs)


def conv_layer(padded, weight_shard):
    return conv_taps(padded, lax.all_gather(weight_shard, "col", axis=3, tiled=True))


def group_total(values, per_group):
    return jnp.sum(values, axis=(0, 1, 2)).reshape(GROUPS, per_group).sum(axis=1)


def norm_silu(values, inner, gain, shift):
    channels = values.shape[3]
    per_group = channels // GROUPS
    members = inner.shape[0] * inner.shape[1] * inner.shape[2] * lax.axis_size("col") * per_group
    chan_sums = group_total(inner, per_group)
    group_mean = lax.psum(chan_sums, "col") / members
    centred = inner - jnp.repeat(group_mean, per_group)
    spread = lax.psum(group_total(centred * centred, per_group), "col") / members
    inv_std = lax.rsqrt(spread + epsilon)
    normed = (values - jnp.repeat(group_mean, per_group)) * jnp.repeat(
        inv_std, per_group
    ) * gain + shift
    return jax.nn.silu(normed).astype(jnp.bfloat16)


def shards(
    latent,
    intersections,
    norm_gain_one,
    norm_shift_one,
    weight_one,
    norm_gain_two,
    norm_shift_two,
    weight_two,
    conv_bias,
):
    source = latent[0]
    latent_full = source.astype(jnp.float32)
    act_one = norm_silu(latent_full, latent_full, norm_gain_one, norm_shift_one)
    margin = extended_2(act_one, (("col", 2),), 2)
    hidden = conv_layer(margin, weight_shard=weight_one).astype(jnp.bfloat16)
    hidden_full = hidden.astype(jnp.float32)
    act_two = norm_silu(hidden_full, hidden_full[:, :, 1:-1], norm_gain_two, norm_shift_two)
    own_width = source.shape[2]
    position = lax.axis_index("col") * own_width - 1 + jnp.arange(own_width + 2, dtype=jnp.int32)
    inside = (position >= 0) & (position < own_width * lax.axis_size("col"))
    act_two = jnp.where(inside[None, None, :, None], act_two, jnp.zeros_like(act_two))
    branch = conv_layer(act_two, weight_shard=weight_two)
    decoded = (latent_full + (branch + conv_bias)).astype(jnp.bfloat16)
    frames = decoded.shape[0]
    received = shifted(decoded[frames - OVMAX :], "tile", 1)
    shared = intersections[0]
    extended = jnp.concatenate([received, jnp.zeros_like(received)], axis=0)
    aligned = lax.dynamic_slice_in_dim(extended, OVMAX - shared, OVMAX, 0)
    position_t = jnp.arange(OVMAX, dtype=jnp.int32)
    own_share = ((position_t + 1).astype(jnp.float32) / (shared + 1).astype(jnp.float32))[
        :, None, None, None
    ]
    head = decoded[:OVMAX].astype(jnp.float32)
    active = (position_t < shared)[:, None, None, None]
    mixed = jnp.where(
        active, own_share * head + (1.0 - own_share) * aligned.astype(jnp.float32), head
    )
    blended = jnp.concatenate([mixed.astype(jnp.bfloat16), decoded[OVMAX:]], axis=0)
    return blended[None]


MESH = pl.DeviceIdType.MESH
LANES = 128


def group_sum(row, per_group):
    lane = lax.broadcasted_iota(jnp.int32, row.shape, 1)
    width = row.shape[1]
    step = 1
    while step < per_group:
        up = pltpu.roll(row, width - step, 1)
        down = pltpu.roll(row, step, 1)
        row = row + jnp.where((lane & step) == 0, up, down)
        step *= 2
    return row


def norm_into(lines, taps, gain, shift, per_group):
    frames = taps.shape[0] - 2
    height, width = taps.shape[1] - 2, taps.shape[2]
    members = frames * height * width * per_group

    def total(f):
        acc = jnp.zeros((8, LANES), jnp.float32)
        for t in range(frames):
            acc = acc + f(lines(t)).reshape(-1, 8, LANES).sum(axis=0)
        row = jnp.broadcast_to(acc.sum(axis=0, keepdims=True), (8, LANES))
        return group_sum(row, per_group)[0:1] / members

    mean = total(lambda v: v)

    def square(v):
        d = v - mean[None]
        return d * d

    scale = lax.rsqrt(total(square) + epsilon)
    where = lax.broadcasted_iota(jnp.int32, (height, width, LANES), 1)
    for t in range(frames):
        v = (lines(t) - mean[None]) * scale[None] * gain[None] + shift[None]
        a = v / (1.0 + jnp.exp(-v))
        left = jnp.where(where == 0, 0.0, pltpu.roll(a, 1, 1))
        right = jnp.where(where == width - 1, 0.0, pltpu.roll(a, width - 1, 1))
        place = (t + 2, pl.ds(1, height))
        taps[place + (slice(None), pl.ds(0, LANES))] = left.astype(jnp.bfloat16)
        taps[place + (slice(None), pl.ds(LANES, LANES))] = a.astype(jnp.bfloat16)
        taps[place + (slice(None), pl.ds(2 * LANES, LANES))] = right.astype(jnp.bfloat16)


def conv_part(taps, weight, first, count, row, rows):
    width, depth = taps.shape[2], taps.shape[3]
    pieces = []
    for dt in range(3):
        for dh in range(3):
            window = taps[pl.ds(first + dt, count), pl.ds(row + dh, rows)]
            pieces.append(window.reshape(count * rows * width, depth))
    lhs = jnp.concatenate(pieces, axis=1)
    rhs = weight[...].reshape(9 * depth, weight.shape[2])
    return jnp.dot(lhs, rhs, preferred_element_type=jnp.float32)


def block_kernel(
    tiles,
    chunks_one,
    chunks_two,
    inter,
    lat,
    gain_one,
    shift_one,
    gain_two,
    shift_two,
    bias,
    w_one,
    w_two,
    out,
    wb_one,
    wb_two,
    got,
    full,
    taps,
    part_out,
    part_in,
    keep_one,
    hid,
    mix_out,
    mix_in,
    keep_two,
    give,
    take,
    tail_in,
    w_local,
    w_send,
    w_recv,
    l_send,
    l_recv,
    p_send,
    p_recv,
    h_send,
    h_recv,
    m_send,
    m_recv,
    g_send,
    g_recv,
    t_send,
    t_recv,
):
    tile = lax.axis_index("tile")
    me = lax.axis_index("col")
    chip = me // 2
    core = me % 2
    partner = chip * 2 + (1 - core)
    twin = (1 - chip) * 2 + core
    frames, height, own_width, channels = lat.shape
    shard = channels // 4
    half = channels // 2
    rows = height // 2
    width = 4 * own_width

    def remote(src, dst, send, recv, col):
        return pltpu.make_async_remote_copy(
            src_ref=src,
            dst_ref=dst,
            send_sem=send,
            recv_sem=recv,
            device_id={"tile": tile, "col": col},
            device_id_type=MESH,
        )

    mine_rows = pl.ds(pl.multiple_of(core * shard, shard), shard)
    w_copies = []
    for k, (w, wb) in enumerate(((w_one, wb_one), (w_two, wb_two))):
        copy = pltpu.make_async_copy(w, wb.at[:, mine_rows, :], w_local.at[k])
        copy.start()
        w_copies.append(copy)

    barrier = pltpu.get_barrier_semaphore()
    for col in (partner, twin):
        pl.semaphore_signal(
            barrier, inc=1, device_id={"tile": tile, "col": col}, device_id_type=MESH
        )

    @pl.when(tile > 0)
    def _():
        pl.semaphore_signal(
            barrier, inc=1, device_id={"tile": tile - 1, "col": me}, device_id_type=MESH
        )

    @pl.when(tile < tiles - 1)
    def _():
        pl.semaphore_signal(
            barrier, inc=1, device_id={"tile": tile + 1, "col": me}, device_id_type=MESH
        )

    pl.semaphore_wait(
        barrier, 2 + jnp.where(tile > 0, 1, 0) + jnp.where(tile < tiles - 1, 1, 0)
    )

    here = pl.ds(pl.multiple_of(chip * half, half), half)
    there = pl.ds(pl.multiple_of((1 - chip) * half, half), half)
    to_twin = remote(lat.at[:, :, :, there], got.at[me], l_send.at[0], l_recv.at[0], twin)
    to_twin.start()
    to_partner = remote(lat.at[:, :, :, here], got.at[me], l_send.at[1], l_recv.at[1], partner)
    to_partner.start()
    w_sends = []
    for k, (w, wb) in enumerate(((w_one, wb_one), (w_two, wb_two))):
        copy = remote(w, wb.at[:, mine_rows, :], w_send.at[k], w_recv.at[k], partner)
        copy.start()
        w_sends.append(copy)

    taps[0:2] = jnp.zeros((2,) + taps.shape[1:], taps.dtype)
    edge = jnp.zeros((frames,) + taps.shape[2:], taps.dtype)
    taps[2:, 0] = edge
    taps[2:, height + 1] = edge

    first_chip = chip == 0
    first_core = core == 0

    def chosen(ref):
        return jnp.where(first_chip, ref[:, :half], ref[:, half:])

    got[me] = jnp.where(first_chip, lat[:, :, :, :half], lat[:, :, :, half:])

    to_twin.wait_recv()
    forward = remote(got.at[twin], got.at[twin], l_send.at[2], l_recv.at[2], partner)
    forward.start()
    to_partner.wait_recv()
    forward.wait_recv()
    for i in range(4):
        full[:, :, i * own_width : (i + 1) * own_width, :] = got[i].astype(jnp.float32)

    per_group = channels // GROUPS
    norm_into(
        lambda t: full[t], taps, chosen(gain_one), chosen(shift_one), per_group
    )

    w_copies[0].wait()
    w_sends[0].wait()
    row = core * rows
    sends = []
    start = 0
    for k, count in enumerate(chunks_one):
        acc = conv_part(taps, wb_one, start, count, row, rows)
        lo, hi = acc[:, :half], acc[:, half:]
        span = pl.ds(start * rows * width, count * rows * width)
        part_out[span] = jnp.where(first_chip, hi, lo).astype(jnp.bfloat16)
        copy = remote(part_out.at[span], part_in.at[span], p_send.at[k], p_recv.at[k], twin)
        copy.start()
        keep_one[span] = jnp.where(first_chip, lo, hi)
        sends.append((copy, span, start, count))
        start += count
    back = []
    for k, (copy, span, first, count) in enumerate(sends):
        copy.wait_recv()
        value = keep_one[span] + part_in[span].astype(jnp.float32)
        place = (pl.ds(first, count), pl.ds(row, rows))
        hid[place] = value.astype(jnp.bfloat16).reshape(count, rows, width, half)
        copy = remote(hid.at[place], hid.at[place], h_send.at[k], h_recv.at[k], partner)
        copy.start()
        back.append(copy)
    for copy in back:
        copy.wait_recv()

    norm_into(
        lambda t: hid[t].astype(jnp.float32), taps, chosen(gain_two), chosen(shift_two), per_group
    )

    w_copies[1].wait()
    w_sends[1].wait()
    cols = 2 * own_width
    sends_two = []
    for k, (first, count) in enumerate(chunks_two):
        acc = conv_part(taps, wb_two, first, count, row, rows)
        acc = acc.reshape(count * rows, width, channels)
        lo, hi = acc[:, :cols], acc[:, cols:]
        span = pl.ds(first * rows * cols, count * rows * cols)
        away = jnp.where(first_chip, hi, lo).reshape(count * rows * cols, channels)
        mix_out[span] = away.astype(jnp.bfloat16)
        copy = remote(mix_out.at[span], mix_in.at[span], m_send.at[k], m_recv.at[k], twin)
        copy.start()
        keep_two[span] = jnp.where(first_chip, lo, hi).reshape(count * rows * cols, channels)
        sends_two.append((copy, span, first, count))

    other_row = (1 - core) * rows
    offset = bias[...][None, None]

    def finish(place, values):
        own = lat[place].astype(jnp.float32)
        out[place] = (own + (values + offset)).astype(jnp.bfloat16)

    overlap = OVMAX
    next_tile = jnp.minimum(tile + 1, tiles - 1)
    tail_copy = pltpu.make_async_remote_copy(
        src_ref=out.at[pl.ds(frames - overlap, overlap)],
        dst_ref=tail_in,
        send_sem=t_send,
        recv_sem=t_recv,
        device_id={"tile": next_tile, "col": me},
        device_id_type=MESH,
    )
    gives = []
    for k, (copy, span, first, count) in enumerate(sends_two):
        copy.wait_recv()
        value = keep_two[span] + mix_in[span].astype(jnp.float32)
        value = value.reshape(count * rows, cols, channels)
        lo, hi = value[:, :own_width], value[:, own_width:]
        times = pl.ds(first, count)
        theirs = jnp.where(first_core, hi, lo)
        give[times] = theirs.reshape(count, rows, own_width, channels)
        swap = remote(give.at[times], take.at[times], g_send.at[k], g_recv.at[k], partner)
        swap.start()
        gives.append(swap)
        ours = jnp.where(first_core, lo, hi).reshape(count, rows, own_width, channels)
        finish((times, pl.ds(row, rows)), ours)
        swap.wait_recv()
        finish((times, pl.ds(other_row, rows)), take[times])
        if k == 0:

            @pl.when(tile < tiles - 1)
            def _():
                tail_copy.start()

    @pl.when(tile > 0)
    def _():
        tail_copy.wait_recv()

    @pl.when(tile == 0)
    def _():
        tail_in[...] = jnp.zeros(tail_in.shape, tail_in.dtype)

    shared = inter[0]
    whole = jnp.full((height, own_width, channels), shared + 1, jnp.int32).astype(jnp.float32)
    for j in range(overlap):
        u = (j + 1) / whole
        before = tail_in[jnp.clip(overlap - shared + j, 0, overlap - 1)].astype(jnp.float32)
        value = out[j].astype(jnp.float32)
        mixed = jnp.where(j < shared, u * value + (1.0 - u) * before, value)
        out[j] = mixed.astype(jnp.bfloat16)

    to_twin.wait_send()
    to_partner.wait_send()
    forward.wait_send()
    for copy, _, _, _ in sends + sends_two:
        copy.wait_send()
    for copy in back + gives:
        copy.wait_send()

    @pl.when(tile < tiles - 1)
    def _():
        tail_copy.wait_send()


def fused(tiles, latent, intersections, gain_one, shift_one, weight_one, gain_two, shift_two, weight_two, bias):
    _, frames, height, own_width, channels = latent.shape
    width, half, rows = 4 * own_width, channels // 2, height // 2
    ahead = (frames + 1) // 2
    chunks_one = (ahead, frames - ahead)
    chunks_two = ((frames - OVMAX, OVMAX), (0, frames - OVMAX))
    shard = weight_one.shape[3]
    vmem = pl.BlockSpec(memory_space=pltpu.VMEM)
    anywhere = pl.BlockSpec(memory_space=pl.ANY)
    spot = frames * rows
    sems = pltpu.SemaphoreType.DMA
    return pl.pallas_call(
        functools.partial(block_kernel, tiles, chunks_one, chunks_two),
        out_shape=jax.ShapeDtypeStruct(latent.shape[1:], jnp.bfloat16),
        in_specs=[pl.BlockSpec(memory_space=pltpu.SMEM)] + [vmem] * 6 + [anywhere] * 2,
        out_specs=vmem,
        scratch_shapes=[
            pltpu.VMEM((27, half, channels), jnp.bfloat16),
            pltpu.VMEM((27, half, channels), jnp.bfloat16),
            pltpu.VMEM((4, frames, height, own_width, half), jnp.bfloat16),
            pltpu.VMEM((frames, height, width, half), jnp.float32),
            pltpu.VMEM((frames + 2, height + 2, width, 3 * half), jnp.bfloat16),
            pltpu.VMEM((spot * width, half), jnp.bfloat16),
            pltpu.VMEM((spot * width, half), jnp.bfloat16),
            pltpu.VMEM((spot * width, half), jnp.float32),
            pltpu.VMEM((frames, height, width, half), jnp.bfloat16),
            pltpu.VMEM((spot * width // 2, channels), jnp.bfloat16),
            pltpu.VMEM((spot * width // 2, channels), jnp.bfloat16),
            pltpu.VMEM((spot * width // 2, channels), jnp.float32),
            pltpu.VMEM((frames, rows, own_width, channels), jnp.float32),
            pltpu.VMEM((frames, rows, own_width, channels), jnp.float32),
            pltpu.VMEM((OVMAX, height, own_width, channels), jnp.bfloat16),
            sems((2,)),
            sems((2,)),
            sems((2,)),
            sems((3,)),
            sems((3,)),
            sems((len(chunks_one),)),
            sems((len(chunks_one),)),
            sems((len(chunks_one),)),
            sems((len(chunks_one),)),
            sems((len(chunks_two),)),
            sems((len(chunks_two),)),
            sems((len(chunks_two),)),
            sems((len(chunks_two),)),
            sems,
            sems,
        ],
        compiler_params=pltpu.CompilerParams(
            collective_id=0, has_side_effects=True, vmem_limit_bytes=60 * 2**20
        ),
    )(
        intersections,
        latent[0],
        gain_one[None],
        shift_one[None],
        gain_two[None],
        shift_two[None],
        bias[None],
        weight_one.reshape(27, shard, channels),
        weight_two.reshape(27, shard, channels),
    )[None]


def program(tiles, cols, *args):
    _, frames, height, own_width, channels = args[0].shape
    fits = (
        cols == 4
        and channels == 2 * LANES
        and own_width == 4
        and height % 2 == 0
        and frames >= 2 * OVMAX
    )
    return fused(tiles, *args) if fits else shards(*args)


def solution(mesh):
    in_specs = (
        P("tile", None, None, "col", None),
        P("tile"),
        P(),
        P(),
        P(None, None, None, "col", None),
        P(),
        P(),
        P(None, None, None, "col", None),
        P(),
    )
    out_specs = P("tile", None, None, "col", None)
    return jax.shard_map(
        functools.partial(program, mesh.shape["tile"], mesh.shape["col"]), mesh=mesh, in_specs=in_specs, out_specs=out_specs, check_vma=False)
```

```python
import functools

import jax
import jax.numpy as jnp
from jax import lax
from jax.experimental import pallas as pl
from jax.experimental.pallas import tpu as pltpu
from jax.sharding import PartitionSpec as P

GROUPS = 32
OVMAX = 4


epsilon = 1e-06


def extended_2(array, sides, width):
    for axis, dim in sides:
        size, length = (lax.axis_size(axis), array.shape[dim])
        up = [(i, (i + 1) % size) for i in range(size - 1)]
        down = [(j, i) for i, j in up]
        last = lax.slice_in_dim(array, length - width, length, axis=dim)
        first = lax.slice_in_dim(array, 0, width, axis=dim)
        before = lax.ppermute(last, axis, up)
        after = lax.ppermute(first, axis, down)
        array = jnp.concatenate([before, array, after], axis=dim)
    return array


def shifted(block, axis, distance):
    devices = range(lax.axis_size(axis))
    route = [(i - distance, i) for i in devices if i - distance in devices]
    return lax.ppermute(block, axis, route)


def conv_taps(padded, kernel):
    frames = padded.shape[0]
    height = padded.shape[1]
    out_width = padded.shape[2] - 2
    channels = padded.shape[3]
    outputs = kernel.shape[4]
    padded = jnp.pad(padded, ((2, 0), (1, 1), (0, 0), (0, 0)))
    running = jnp.zeros((frames * height * out_width, outputs), jnp.float32)
    for tap_t in range(3):
        for tap_h in range(3):
            for tap_w in range(3):
                window = padded[
                    tap_t : tap_t + frames, tap_h : tap_h + height, tap_w : tap_w + out_width
                ]
                running = running + jnp.dot(
                    window.reshape(-1, channels),
                    kernel[tap_t, tap_h, tap_w],
                    preferred_element_type=jnp.float32,
                )
    return running.reshape(frames, height, out_width, outputs)


def conv_layer(padded, weight_shard):
    return conv_taps(padded, lax.all_gather(weight_shard, "col", axis=3, tiled=True))


def group_total(values, per_group):
    return jnp.sum(values, axis=(0, 1, 2)).reshape(GROUPS, per_group).sum(axis=1)


def norm_silu(values, inner, gain, shift):
    channels = values.shape[3]
    per_group = channels // GROUPS
    members = inner.shape[0] * inner.shape[1] * inner.shape[2] * lax.axis_size("col") * per_group
    chan_sums = group_total(inner, per_group)
    group_mean = lax.psum(chan_sums, "col") / members
    centred = inner - jnp.repeat(group_mean, per_group)
    spread = lax.psum(group_total(centred * centred, per_group), "col") / members
    inv_std = lax.rsqrt(spread + epsilon)
    normed = (values - jnp.repeat(group_mean, per_group)) * jnp.repeat(
        inv_std, per_group
    ) * gain + shift
    return jax.nn.silu(normed).astype(jnp.bfloat16)


def shards(
    latent,
    intersections,
    norm_gain_one,
    norm_shift_one,
    weight_one,
    norm_gain_two,
    norm_shift_two,
    weight_two,
    conv_bias,
):
    source = latent[0]
    latent_full = source.astype(jnp.float32)
    act_one = norm_silu(latent_full, latent_full, norm_gain_one, norm_shift_one)
    margin = extended_2(act_one, (("col", 2),), 2)
    hidden = conv_layer(margin, weight_shard=weight_one).astype(jnp.bfloat16)
    hidden_full = hidden.astype(jnp.float32)
    act_two = norm_silu(hidden_full, hidden_full[:, :, 1:-1], norm_gain_two, norm_shift_two)
    own_width = source.shape[2]
    position = lax.axis_index("col") * own_width - 1 + jnp.arange(own_width + 2, dtype=jnp.int32)
    inside = (position >= 0) & (position < own_width * lax.axis_size("col"))
    act_two = jnp.where(inside[None, None, :, None], act_two, jnp.zeros_like(act_two))
    branch = conv_layer(act_two, weight_shard=weight_two)
    decoded = (latent_full + (branch + conv_bias)).astype(jnp.bfloat16)
    frames = decoded.shape[0]
    received = shifted(decoded[frames - OVMAX :], "tile", 1)
    shared = intersections[0]
    extended = jnp.concatenate([received, jnp.zeros_like(received)], axis=0)
    aligned = lax.dynamic_slice_in_dim(extended, OVMAX - shared, OVMAX, 0)
    position_t = jnp.arange(OVMAX, dtype=jnp.int32)
    own_share = ((position_t + 1).astype(jnp.float32) / (shared + 1).astype(jnp.float32))[
        :, None, None, None
    ]
    head = decoded[:OVMAX].astype(jnp.float32)
    active = (position_t < shared)[:, None, None, None]
    mixed = jnp.where(
        active, own_share * head + (1.0 - own_share) * aligned.astype(jnp.float32), head
    )
    blended = jnp.concatenate([mixed.astype(jnp.bfloat16), decoded[OVMAX:]], axis=0)
    return blended[None]


MESH = pl.DeviceIdType.MESH
LANES = 128


def group_sum(row, per_group):
    lane = lax.broadcasted_iota(jnp.int32, row.shape, 1)
    width = row.shape[1]
    step = 1
    while step < per_group:
        up = pltpu.roll(row, width - step, 1)
        down = pltpu.roll(row, step, 1)
        row = row + jnp.where((lane & step) == 0, up, down)
        step *= 2
    return row


def norm_into(frames, lines, store, gain, shift, per_group):
    height, width, _ = lines(0).shape
    members = frames * height * width * per_group

    def total(f):
        acc = jnp.zeros((8, LANES), jnp.float32)
        for t in range(frames):
            acc = acc + f(lines(t)).reshape(-1, 8, LANES).sum(axis=0)
        row = jnp.broadcast_to(acc.sum(axis=0, keepdims=True), (8, LANES))
        return group_sum(row, per_group)[0:1] / members

    mean = total(lambda v: v)

    def square(v):
        d = v - mean[None]
        return d * d

    scale = lax.rsqrt(total(square) + epsilon)
    where = lax.broadcasted_iota(jnp.int32, (height, width, LANES), 1)
    for t in range(frames):
        v = (lines(t) - mean[None]) * scale[None] * gain[None] + shift[None]
        a = v / (1.0 + jnp.exp(-v))
        left = jnp.where(where == 0, 0.0, pltpu.roll(a, 1, 1))
        right = jnp.where(where == width - 1, 0.0, pltpu.roll(a, width - 1, 1))
        store(t, (left, a, right))


def conv_part(taps, weight, first, count, row, rows):
    width, depth = taps.shape[2], taps.shape[3]
    pieces = []
    for dt in range(3):
        for dh in range(3):
            window = taps[pl.ds(first + dt, count), pl.ds(row + dh, rows)]
            pieces.append(window.reshape(count * rows * width, depth))
    lhs = jnp.concatenate(pieces, axis=1)
    rhs = weight[...].reshape(9 * depth, weight.shape[2])
    return jnp.dot(lhs, rhs, preferred_element_type=jnp.float32)


def conv_packed(taps, weight, first, count):
    rows, depth = taps.shape[1], taps.shape[2]
    pieces = [taps[pl.ds(first + dt, count)].reshape(count * rows, depth) for dt in range(3)]
    lhs = jnp.concatenate(pieces, axis=1)
    rhs = weight[...].reshape(3 * depth, weight.shape[2])
    return jnp.dot(lhs, rhs, preferred_element_type=jnp.float32)


def block_kernel(
    tiles,
    chunks_one,
    chunks_two,
    inter_hbm,
    lat_hbm,
    gain_one_hbm,
    shift_one_hbm,
    gain_two_hbm,
    shift_two_hbm,
    bias_hbm,
    w_one,
    w_two,
    out,
    inter,
    lat,
    small,
    wb_one,
    wb_two,
    got,
    full,
    taps,
    packed,
    part_out,
    part_in,
    keep_one,
    hid,
    mix_out,
    mix_in,
    keep_two,
    tail_in,
    in_sem,
    w_local,
    w_send,
    w_recv,
    l_send,
    l_recv,
    p_send,
    p_recv,
    h_send,
    h_recv,
    m_send,
    m_recv,
    t_send,
    t_recv,
):
    tile = lax.axis_index("tile")
    me = lax.axis_index("col")
    chip = me // 2
    core = me % 2
    partner = chip * 2 + (1 - core)
    twin = (1 - chip) * 2 + core
    frames, height, own_width, channels = lat.shape
    shard = channels // 4
    half = channels // 2
    rows = height // 2
    width = 4 * own_width

    def remote(src, dst, send, recv, col):
        return pltpu.make_async_remote_copy(
            src_ref=src,
            dst_ref=dst,
            send_sem=send,
            recv_sem=recv,
            device_id={"tile": tile, "col": col},
            device_id_type=MESH,
        )

    barrier = pltpu.get_barrier_semaphore()
    for col in (partner, twin):
        pl.semaphore_signal(
            barrier, inc=1, device_id={"tile": tile, "col": col}, device_id_type=MESH
        )

    @pl.when(tile > 0)
    def _():
        pl.semaphore_signal(
            barrier, inc=1, device_id={"tile": tile - 1, "col": me}, device_id_type=MESH
        )

    @pl.when(tile < tiles - 1)
    def _():
        pl.semaphore_signal(
            barrier, inc=1, device_id={"tile": tile + 1, "col": me}, device_id_type=MESH
        )

    lat_copy = pltpu.make_async_copy(lat_hbm, lat, in_sem.at[0])
    lat_copy.start()
    vectors = (gain_one_hbm, shift_one_hbm, gain_two_hbm, shift_two_hbm, bias_hbm)
    loads = [pltpu.make_async_copy(inter_hbm, inter, in_sem.at[1])]
    for k, vector in enumerate(vectors):
        loads.append(pltpu.make_async_copy(vector, small.at[k], in_sem.at[2 + k]))
    for copy in loads:
        copy.start()
    mine_rows = pl.ds(pl.multiple_of(core * shard, shard), shard)
    w_copies = []
    for k, (w, wb) in enumerate(((w_one, wb_one), (w_two, wb_two))):
        copy = pltpu.make_async_copy(w, wb.at[:, mine_rows, :], w_local.at[k])
        copy.start()
        w_copies.append(copy)

    first_chip = chip == 0
    first_core = core == 0
    here = pl.ds(pl.multiple_of(chip * half, half), half)
    there = pl.ds(pl.multiple_of((1 - chip) * half, half), half)
    to_twin = remote(lat.at[:, :, :, there], got.at[me], l_send.at[0], l_recv.at[0], twin)
    to_partner = remote(lat.at[:, :, :, here], got.at[me], l_send.at[1], l_recv.at[1], partner)
    forward = remote(got.at[twin], got.at[twin], l_send.at[2], l_recv.at[2], partner)
    w_sends = [
        remote(w, wb.at[:, mine_rows, :], w_send.at[k], w_recv.at[k], partner)
        for k, (w, wb) in enumerate(((w_one, wb_one), (w_two, wb_two)))
    ]

    lat_copy.wait()
    pl.semaphore_wait(
        barrier, 2 + jnp.where(tile > 0, 1, 0) + jnp.where(tile < tiles - 1, 1, 0)
    )
    to_twin.start()
    to_partner.start()
    w_sends[0].start()

    got[me] = jnp.where(first_chip, lat[:, :, :, :half], lat[:, :, :, half:])
    taps[0:2] = jnp.zeros((2,) + taps.shape[1:], taps.dtype)
    edge = jnp.zeros((frames,) + taps.shape[2:], taps.dtype)
    taps[2:, 0] = edge
    taps[2:, height + 1] = edge
    packed[0:2] = jnp.zeros((2,) + packed.shape[1:], packed.dtype)

    for copy in loads:
        copy.wait()

    def chosen(k):
        return jnp.where(first_chip, small[k][:, :half], small[k][:, half:])

    def store_taps(t, three):
        for k, value in enumerate(three):
            place = (t + 2, pl.ds(1, height), slice(None), pl.ds(k * LANES, LANES))
            taps[place] = value.astype(jnp.bfloat16)

    cols = 2 * own_width
    sub = lax.broadcasted_iota(jnp.int32, (height, cols, LANES), 1)

    def store_packed(t, three):
        zero = jnp.zeros((1, cols, LANES), jnp.float32)
        for k, value in enumerate(three):
            lo, hi = value[:, :cols], value[:, cols:]
            low = jnp.where(first_core, lo, pltpu.roll(lo, own_width, 1))
            high = jnp.where(first_core, pltpu.roll(hi, own_width, 1), hi)
            line = jnp.where(sub < own_width, low, high)
            moved = (
                jnp.concatenate([zero, line[:-1]], axis=0),
                line,
                jnp.concatenate([line[1:], zero], axis=0),
            )
            for dh, lines in enumerate(moved):
                value = lines.reshape(height * cols, LANES).astype(jnp.bfloat16)
                packed[t + 2, :, pl.ds((dh * 3 + k) * LANES, LANES)] = value

    to_twin.wait_recv()
    forward.start()
    w_sends[1].start()
    to_partner.wait_recv()
    forward.wait_recv()
    for i in range(4):
        full[:, :, i * own_width : (i + 1) * own_width, :] = got[i].astype(jnp.float32)

    per_group = channels // GROUPS
    norm_into(frames, lambda t: full[t], store_taps, chosen(0), chosen(1), per_group)

    w_copies[0].wait()
    w_sends[0].wait()
    row = core * rows
    sends = []
    start = 0
    for k, count in enumerate(chunks_one):
        acc = conv_part(taps, wb_one, start, count, row, rows)
        lo, hi = acc[:, :half], acc[:, half:]
        span = pl.ds(start * rows * width, count * rows * width)
        part_out[span] = jnp.where(first_chip, hi, lo).astype(jnp.bfloat16)
        copy = remote(part_out.at[span], part_in.at[span], p_send.at[k], p_recv.at[k], twin)
        copy.start()
        keep_one[span] = jnp.where(first_chip, lo, hi)
        sends.append((copy, span, start, count))
        start += count
    back = []
    for k, (copy, span, first, count) in enumerate(sends):
        copy.wait_recv()
        value = keep_one[span] + part_in[span].astype(jnp.float32)
        place = (pl.ds(first, count), pl.ds(row, rows))
        hid[place] = value.astype(jnp.bfloat16).reshape(count, rows, width, half)
        copy = remote(hid.at[place], hid.at[place], h_send.at[k], h_recv.at[k], partner)
        copy.start()
        back.append(copy)
    for copy in back:
        copy.wait_recv()

    norm_into(
        frames,
        lambda t: hid[t].astype(jnp.float32),
        store_packed,
        chosen(2),
        chosen(3),
        per_group,
    )

    w_copies[1].wait()
    w_sends[1].wait()
    offset = small[4][None, None]
    sends_two = []
    for k, (first, count) in enumerate(chunks_two):
        acc = conv_packed(packed, wb_two, first, count)
        acc = acc.reshape(count, height, cols, channels)
        lo, hi = acc[:, :, :own_width], acc[:, :, own_width:]
        times = pl.ds(first, count)
        mix_out[times] = jnp.where(first_chip, hi, lo).astype(jnp.bfloat16)
        copy = remote(mix_out.at[times], mix_in.at[times], m_send.at[k], m_recv.at[k], twin)
        copy.start()
        own = jnp.where(first_chip, lo, hi)
        keep_two[times] = lat[times].astype(jnp.float32) + (own + offset)
        sends_two.append((copy, times))

    overlap = OVMAX
    next_tile = jnp.minimum(tile + 1, tiles - 1)
    tail_copy = pltpu.make_async_remote_copy(
        src_ref=out.at[pl.ds(frames - overlap, overlap)],
        dst_ref=tail_in,
        send_sem=t_send,
        recv_sem=t_recv,
        device_id={"tile": next_tile, "col": me},
        device_id_type=MESH,
    )
    for k, (copy, times) in enumerate(sends_two):
        copy.wait_recv()
        value = keep_two[times] + mix_in[times].astype(jnp.float32)
        out[times] = value.astype(jnp.bfloat16)
        if k == 0:

            @pl.when(tile < tiles - 1)
            def _():
                tail_copy.start()

    @pl.when(tile > 0)
    def _():
        tail_copy.wait_recv()

    @pl.when(tile == 0)
    def _():
        tail_in[...] = jnp.zeros(tail_in.shape, tail_in.dtype)

    shared = inter[0]
    whole = jnp.full((height, own_width, channels), shared + 1, jnp.int32).astype(jnp.float32)
    for j in range(overlap):
        u = (j + 1) / whole
        before = tail_in[jnp.clip(overlap - shared + j, 0, overlap - 1)].astype(jnp.float32)
        value = out[j].astype(jnp.float32)
        mixed = jnp.where(j < shared, u * value + (1.0 - u) * before, value)
        out[j] = mixed.astype(jnp.bfloat16)

    to_twin.wait_send()
    to_partner.wait_send()
    forward.wait_send()
    for copy, *_ in sends + sends_two:
        copy.wait_send()
    for copy in back:
        copy.wait_send()

    @pl.when(tile < tiles - 1)
    def _():
        tail_copy.wait_send()


def fused(tiles, latent, intersections, gain_one, shift_one, weight_one, gain_two, shift_two, weight_two, bias):
    _, frames, height, own_width, channels = latent.shape
    width, half, rows = 4 * own_width, channels // 2, height // 2
    early = frames // 4
    middle = (frames - early) // 2
    chunks_one = (early, middle, frames - early - middle)
    rest = frames - OVMAX
    chunks_two = ((rest, OVMAX), (0, rest // 2), (rest // 2, rest - rest // 2))
    shard = weight_one.shape[3]
    anywhere = pl.BlockSpec(memory_space=pl.ANY)
    spot = frames * rows
    sems = pltpu.SemaphoreType.DMA
    own_block = latent.shape[1:]
    return pl.pallas_call(
        functools.partial(block_kernel, tiles, chunks_one, chunks_two),
        out_shape=pltpu.VMEM(own_block, jnp.bfloat16),
        in_specs=[pl.BlockSpec(memory_space=pltpu.HBM)] * 9,
        out_specs=pl.BlockSpec(memory_space=pltpu.VMEM),
        scratch_shapes=[
            pltpu.SMEM((1,), jnp.int32),
            pltpu.VMEM(own_block, jnp.bfloat16),
            pltpu.VMEM((5, 1, channels), jnp.float32),
            pltpu.VMEM((27, half, channels), jnp.bfloat16),
            pltpu.VMEM((27, half, channels), jnp.bfloat16),
            pltpu.VMEM((4, frames, height, own_width, half), jnp.bfloat16),
            pltpu.VMEM((frames, height, width, half), jnp.float32),
            pltpu.VMEM((frames + 2, height + 2, width, 3 * half), jnp.bfloat16),
            pltpu.VMEM((frames + 2, height * 2 * own_width, 9 * half), jnp.bfloat16),
            pltpu.VMEM((spot * width, half), jnp.bfloat16),
            pltpu.VMEM((spot * width, half), jnp.bfloat16),
            pltpu.VMEM((spot * width, half), jnp.float32),
            pltpu.VMEM((frames, height, width, half), jnp.bfloat16),
            pltpu.VMEM(own_block, jnp.bfloat16),
            pltpu.VMEM(own_block, jnp.bfloat16),
            pltpu.VMEM(own_block, jnp.float32),
            pltpu.VMEM((OVMAX,) + own_block[1:], jnp.bfloat16),
            sems((7,)),
            sems((2,)),
            sems((2,)),
            sems((2,)),
            sems((3,)),
            sems((3,)),
            sems((len(chunks_one),)),
            sems((len(chunks_one),)),
            sems((len(chunks_one),)),
            sems((len(chunks_one),)),
            sems((len(chunks_two),)),
            sems((len(chunks_two),)),
            sems,
            sems,
        ],
        compiler_params=pltpu.CompilerParams(
            collective_id=0, has_side_effects=True, vmem_limit_bytes=60 * 2**20
        ),
    )(
        intersections,
        latent[0],
        gain_one[None],
        shift_one[None],
        gain_two[None],
        shift_two[None],
        bias[None],
        weight_one.reshape(27, shard, channels),
        weight_two.reshape(27, shard, channels),
    )[None]


def program(tiles, cols, *args):
    _, frames, height, own_width, channels = args[0].shape
    fits = (
        cols == 4
        and channels == 2 * LANES
        and own_width == 4
        and height % 2 == 0
        and frames >= 2 * OVMAX
    )
    return fused(tiles, *args) if fits else shards(*args)


def solution(mesh):
    in_specs = (
        P("tile", None, None, "col", None),
        P("tile"),
        P(),
        P(),
        P(None, None, None, "col", None),
        P(),
        P(),
        P(None, None, None, "col", None),
        P(),
    )
    out_specs = P("tile", None, None, "col", None)
    return jax.shard_map(
        functools.partial(program, mesh.shape["tile"], mesh.shape["col"]), mesh=mesh, in_specs=in_specs, out_specs=out_specs, check_vma=False)
```

```python
import functools

import jax
import jax.numpy as jnp
from jax import lax
from jax.experimental import pallas as pl
from jax.experimental.pallas import tpu as pltpu
from jax.sharding import PartitionSpec as P

GROUPS = 32
OVMAX = 4


epsilon = 1e-06


def extended_2(array, sides, width):
    for axis, dim in sides:
        size, length = (lax.axis_size(axis), array.shape[dim])
        up = [(i, (i + 1) % size) for i in range(size - 1)]
        down = [(j, i) for i, j in up]
        last = lax.slice_in_dim(array, length - width, length, axis=dim)
        first = lax.slice_in_dim(array, 0, width, axis=dim)
        before = lax.ppermute(last, axis, up)
        after = lax.ppermute(first, axis, down)
        array = jnp.concatenate([before, array, after], axis=dim)
    return array


def shifted(block, axis, distance):
    devices = range(lax.axis_size(axis))
    route = [(i - distance, i) for i in devices if i - distance in devices]
    return lax.ppermute(block, axis, route)


def conv_taps(padded, kernel):
    frames = padded.shape[0]
    height = padded.shape[1]
    out_width = padded.shape[2] - 2
    channels = padded.shape[3]
    outputs = kernel.shape[4]
    padded = jnp.pad(padded, ((2, 0), (1, 1), (0, 0), (0, 0)))
    running = jnp.zeros((frames * height * out_width, outputs), jnp.float32)
    for tap_t in range(3):
        for tap_h in range(3):
            for tap_w in range(3):
                window = padded[
                    tap_t : tap_t + frames, tap_h : tap_h + height, tap_w : tap_w + out_width
                ]
                running = running + jnp.dot(
                    window.reshape(-1, channels),
                    kernel[tap_t, tap_h, tap_w],
                    preferred_element_type=jnp.float32,
                )
    return running.reshape(frames, height, out_width, outputs)


def conv_layer(padded, weight_shard):
    return conv_taps(padded, lax.all_gather(weight_shard, "col", axis=3, tiled=True))


def group_total(values, per_group):
    return jnp.sum(values, axis=(0, 1, 2)).reshape(GROUPS, per_group).sum(axis=1)


def norm_silu(values, inner, gain, shift):
    channels = values.shape[3]
    per_group = channels // GROUPS
    members = inner.shape[0] * inner.shape[1] * inner.shape[2] * lax.axis_size("col") * per_group
    chan_sums = group_total(inner, per_group)
    group_mean = lax.psum(chan_sums, "col") / members
    centred = inner - jnp.repeat(group_mean, per_group)
    spread = lax.psum(group_total(centred * centred, per_group), "col") / members
    inv_std = lax.rsqrt(spread + epsilon)
    normed = (values - jnp.repeat(group_mean, per_group)) * jnp.repeat(
        inv_std, per_group
    ) * gain + shift
    return jax.nn.silu(normed).astype(jnp.bfloat16)


def shards(
    latent,
    intersections,
    norm_gain_one,
    norm_shift_one,
    weight_one,
    norm_gain_two,
    norm_shift_two,
    weight_two,
    conv_bias,
):
    source = latent[0]
    latent_full = source.astype(jnp.float32)
    act_one = norm_silu(latent_full, latent_full, norm_gain_one, norm_shift_one)
    margin = extended_2(act_one, (("col", 2),), 2)
    hidden = conv_layer(margin, weight_shard=weight_one).astype(jnp.bfloat16)
    hidden_full = hidden.astype(jnp.float32)
    act_two = norm_silu(hidden_full, hidden_full[:, :, 1:-1], norm_gain_two, norm_shift_two)
    own_width = source.shape[2]
    position = lax.axis_index("col") * own_width - 1 + jnp.arange(own_width + 2, dtype=jnp.int32)
    inside = (position >= 0) & (position < own_width * lax.axis_size("col"))
    act_two = jnp.where(inside[None, None, :, None], act_two, jnp.zeros_like(act_two))
    branch = conv_layer(act_two, weight_shard=weight_two)
    decoded = (latent_full + (branch + conv_bias)).astype(jnp.bfloat16)
    frames = decoded.shape[0]
    received = shifted(decoded[frames - OVMAX :], "tile", 1)
    shared = intersections[0]
    extended = jnp.concatenate([received, jnp.zeros_like(received)], axis=0)
    aligned = lax.dynamic_slice_in_dim(extended, OVMAX - shared, OVMAX, 0)
    position_t = jnp.arange(OVMAX, dtype=jnp.int32)
    own_share = ((position_t + 1).astype(jnp.float32) / (shared + 1).astype(jnp.float32))[
        :, None, None, None
    ]
    head = decoded[:OVMAX].astype(jnp.float32)
    active = (position_t < shared)[:, None, None, None]
    mixed = jnp.where(
        active, own_share * head + (1.0 - own_share) * aligned.astype(jnp.float32), head
    )
    blended = jnp.concatenate([mixed.astype(jnp.bfloat16), decoded[OVMAX:]], axis=0)
    return blended[None]


MESH = pl.DeviceIdType.MESH
LANES = 128


def group_sum(row, per_group):
    lane = lax.broadcasted_iota(jnp.int32, row.shape, 1)
    width = row.shape[1]
    step = 1
    while step < per_group:
        up = pltpu.roll(row, width - step, 1)
        down = pltpu.roll(row, step, 1)
        row = row + jnp.where((lane & step) == 0, up, down)
        step *= 2
    return row


def norm_of(frames, lines, store, gain, shift, per_group):
    height, width, _ = lines(0).shape
    members = frames * height * width * per_group

    def total(f):
        acc = jnp.zeros((8, LANES), jnp.float32)
        for t in range(frames):
            acc = acc + f(lines(t)).reshape(-1, 8, LANES).sum(axis=0)
        row = jnp.broadcast_to(acc.sum(axis=0, keepdims=True), (8, LANES))
        return group_sum(row, per_group)[0:1] / members

    mean = total(lambda v: v)

    def square(v):
        d = v - mean[None]
        return d * d

    scale = lax.rsqrt(total(square) + epsilon)
    where = lax.broadcasted_iota(jnp.int32, (height, width, LANES), 1)
    factor = scale * gain

    def normalise(times):
        for t in times:
            v = (lines(t) - mean[None]) * factor[None] + shift[None]
            b = 0.5 * v
            a = b + b * jnp.tanh(b)
            left = jnp.where(where == 0, 0.0, pltpu.roll(a, 1, 1))
            right = jnp.where(where == width - 1, 0.0, pltpu.roll(a, width - 1, 1))
            store(t, (left, a, right))

    return normalise


def conv_part(taps, weight, first, count, row, rows):
    width, depth = taps.shape[2], taps.shape[3]
    pieces = []
    for dt in range(3):
        for dh in range(3):
            window = taps[pl.ds(first + dt, count), pl.ds(row + dh, rows)]
            pieces.append(window.reshape(count * rows * width, depth))
    lhs = jnp.concatenate(pieces, axis=1)
    rhs = weight[...].reshape(9 * depth, weight.shape[2])
    return jnp.dot(lhs, rhs, preferred_element_type=jnp.float32)


def conv_packed(taps, weight, first, count):
    rows, depth = taps.shape[1], taps.shape[2]
    pieces = [taps[pl.ds(first + dt, count)].reshape(count * rows, depth) for dt in range(3)]
    lhs = jnp.concatenate(pieces, axis=1)
    rhs = weight[...].reshape(3 * depth, weight.shape[2])
    return jnp.dot(lhs, rhs, preferred_element_type=jnp.float32)


def block_kernel(
    tiles,
    chunks_one,
    chunks_two,
    inter_hbm,
    lat_hbm,
    gain_one_hbm,
    shift_one_hbm,
    gain_two_hbm,
    shift_two_hbm,
    bias_hbm,
    w_one,
    w_two,
    out,
    inter,
    lat,
    small,
    wb_one,
    wb_two,
    got,
    full,
    taps,
    packed,
    part_out,
    part_in,
    keep_one,
    hid,
    mix_out,
    mix_in,
    keep_two,
    tail_in,
    in_sem,
    w_local,
    w_send,
    w_recv,
    l_send,
    l_recv,
    p_send,
    p_recv,
    h_send,
    h_recv,
    m_send,
    m_recv,
    t_send,
    t_recv,
):
    tile = lax.axis_index("tile")
    me = lax.axis_index("col")
    chip = me // 2
    core = me % 2
    partner = chip * 2 + (1 - core)
    twin = (1 - chip) * 2 + core
    frames, height, own_width, channels = lat.shape
    shard = channels // 4
    half = channels // 2
    rows = height // 2
    width = 4 * own_width

    def remote(src, dst, send, recv, col):
        return pltpu.make_async_remote_copy(
            src_ref=src,
            dst_ref=dst,
            send_sem=send,
            recv_sem=recv,
            device_id={"tile": tile, "col": col},
            device_id_type=MESH,
        )

    barrier = pltpu.get_barrier_semaphore()
    for col in (partner, twin):
        pl.semaphore_signal(
            barrier, inc=1, device_id={"tile": tile, "col": col}, device_id_type=MESH
        )

    @pl.when(tile > 0)
    def _():
        pl.semaphore_signal(
            barrier, inc=1, device_id={"tile": tile - 1, "col": me}, device_id_type=MESH
        )

    lat_copy = pltpu.make_async_copy(lat_hbm, lat, in_sem.at[0])
    lat_copy.start()
    vectors = (gain_one_hbm, shift_one_hbm, gain_two_hbm, shift_two_hbm, bias_hbm)
    loads = [pltpu.make_async_copy(inter_hbm, inter, in_sem.at[1])]
    for k, vector in enumerate(vectors):
        loads.append(pltpu.make_async_copy(vector, small.at[k], in_sem.at[2 + k]))
    for copy in loads:
        copy.start()
    mine_rows = pl.ds(pl.multiple_of(core * shard, shard), shard)
    w_copies = []
    for k, (w, wb) in enumerate(((w_one, wb_one), (w_two, wb_two))):
        copy = pltpu.make_async_copy(w, wb.at[:, mine_rows, :], w_local.at[k])
        copy.start()
        w_copies.append(copy)

    first_chip = chip == 0
    first_core = core == 0
    here = pl.ds(pl.multiple_of(chip * half, half), half)
    there = pl.ds(pl.multiple_of((1 - chip) * half, half), half)
    to_twin = remote(lat.at[:, :, :, there], got.at[me], l_send.at[0], l_recv.at[0], twin)
    to_partner = remote(lat.at[:, :, :, here], got.at[me], l_send.at[1], l_recv.at[1], partner)
    forward = remote(got.at[twin], got.at[twin], l_send.at[2], l_recv.at[2], partner)
    w_sends = [
        remote(w, wb.at[:, mine_rows, :], w_send.at[k], w_recv.at[k], partner)
        for k, (w, wb) in enumerate(((w_one, wb_one), (w_two, wb_two)))
    ]

    lat_copy.wait()
    pl.semaphore_wait(barrier, 2 + jnp.where(tile < tiles - 1, 1, 0))
    to_twin.start()
    to_partner.start()
    w_sends[0].start()

    got[me] = jnp.where(first_chip, lat[:, :, :, :half], lat[:, :, :, half:])
    taps[0:2] = jnp.zeros((2,) + taps.shape[1:], taps.dtype)
    edge = jnp.zeros((frames,) + taps.shape[2:], taps.dtype)
    taps[2:, 0] = edge
    taps[2:, height + 1] = edge
    packed[0:2] = jnp.zeros((2,) + packed.shape[1:], packed.dtype)

    for copy in loads:
        copy.wait()

    def chosen(k):
        return jnp.where(first_chip, small[k][:, :half], small[k][:, half:])

    def store_taps(t, three):
        for k, value in enumerate(three):
            place = (t + 2, pl.ds(1, height), slice(None), pl.ds(k * LANES, LANES))
            taps[place] = value.astype(jnp.bfloat16)

    cols = 2 * own_width
    sub = lax.broadcasted_iota(jnp.int32, (height, cols, LANES), 1)

    def store_packed(t, three):
        zero = jnp.zeros((1, cols, LANES), jnp.float32)
        for k, value in enumerate(three):
            lo, hi = value[:, :cols], value[:, cols:]
            low = jnp.where(first_core, lo, pltpu.roll(lo, own_width, 1))
            high = jnp.where(first_core, pltpu.roll(hi, own_width, 1), hi)
            line = jnp.where(sub < own_width, low, high)
            moved = (
                jnp.concatenate([zero, line[:-1]], axis=0),
                line,
                jnp.concatenate([line[1:], zero], axis=0),
            )
            for dh, lines in enumerate(moved):
                value = lines.reshape(height * cols, LANES).astype(jnp.bfloat16)
                packed[t + 2, :, pl.ds((dh * 3 + k) * LANES, LANES)] = value

    to_twin.wait_recv()
    forward.start()
    w_sends[1].start()
    to_partner.wait_recv()
    forward.wait_recv()
    for i in range(4):
        full[:, :, i * own_width : (i + 1) * own_width, :] = got[i].astype(jnp.float32)

    per_group = channels // GROUPS
    normalise = norm_of(frames, lambda t: full[t], store_taps, chosen(0), chosen(1), per_group)

    row = core * rows
    sends = []
    start = 0
    for k, count in enumerate(chunks_one):
        normalise(range(start, start + count))
        if k == 0:
            w_copies[0].wait()
            w_sends[0].wait()
        acc = conv_part(taps, wb_one, start, count, row, rows)
        lo, hi = acc[:, :half], acc[:, half:]
        span = pl.ds(start * rows * width, count * rows * width)
        part_out[span] = jnp.where(first_chip, hi, lo).astype(jnp.bfloat16)
        copy = remote(part_out.at[span], part_in.at[span], p_send.at[k], p_recv.at[k], twin)
        copy.start()
        keep_one[span] = jnp.where(first_chip, lo, hi)
        sends.append((copy, span, start, count))
        start += count
    back = []
    for k, (copy, span, first, count) in enumerate(sends):
        copy.wait_recv()
        value = keep_one[span] + part_in[span].astype(jnp.float32)
        place = (pl.ds(first, count), pl.ds(row, rows))
        hid[place] = value.astype(jnp.bfloat16).reshape(count, rows, width, half)
        copy = remote(hid.at[place], hid.at[place], h_send.at[k], h_recv.at[k], partner)
        copy.start()
        back.append(copy)
    for copy in back:
        copy.wait_recv()

    normalise = norm_of(
        frames,
        lambda t: hid[t].astype(jnp.float32),
        store_packed,
        chosen(2),
        chosen(3),
        per_group,
    )

    done = set()
    offset = small[4][None, None]
    sends_two = []
    for k, (first, count) in enumerate(chunks_two):
        needed = [t for t in range(max(first - 2, 0), first + count) if t not in done]
        normalise(needed)
        done.update(needed)
        if k == 0:
            w_copies[1].wait()
            w_sends[1].wait()
        acc = conv_packed(packed, wb_two, first, count)
        acc = acc.reshape(count, height, cols, channels)
        lo, hi = acc[:, :, :own_width], acc[:, :, own_width:]
        times = pl.ds(first, count)
        mix_out[times] = jnp.where(first_chip, hi, lo).astype(jnp.bfloat16)
        copy = remote(mix_out.at[times], mix_in.at[times], m_send.at[k], m_recv.at[k], twin)
        copy.start()
        own = jnp.where(first_chip, lo, hi)
        keep_two[times] = lat[times].astype(jnp.float32) + (own + offset)
        sends_two.append((copy, times))

    overlap = OVMAX
    next_tile = jnp.minimum(tile + 1, tiles - 1)
    tail_copy = pltpu.make_async_remote_copy(
        src_ref=out.at[pl.ds(frames - overlap, overlap)],
        dst_ref=tail_in,
        send_sem=t_send,
        recv_sem=t_recv,
        device_id={"tile": next_tile, "col": me},
        device_id_type=MESH,
    )
    for k, (copy, times) in enumerate(sends_two):
        copy.wait_recv()
        value = keep_two[times] + mix_in[times].astype(jnp.float32)
        out[times] = value.astype(jnp.bfloat16)
        if k == 0:

            @pl.when(tile < tiles - 1)
            def _():
                tail_copy.start()

    @pl.when(tile > 0)
    def _():
        tail_copy.wait_recv()

    @pl.when(tile == 0)
    def _():
        tail_in[...] = jnp.zeros(tail_in.shape, tail_in.dtype)

    shared = inter[0]
    whole = jnp.full((height, own_width, channels), shared + 1, jnp.int32).astype(jnp.float32)
    for j in range(overlap):
        u = (j + 1) / whole
        before = tail_in[jnp.clip(overlap - shared + j, 0, overlap - 1)].astype(jnp.float32)
        value = out[j].astype(jnp.float32)
        mixed = jnp.where(j < shared, u * value + (1.0 - u) * before, value)
        out[j] = mixed.astype(jnp.bfloat16)

    to_twin.wait_send()
    to_partner.wait_send()
    forward.wait_send()
    for copy, *_ in sends + sends_two:
        copy.wait_send()
    for copy in back:
        copy.wait_send()

    @pl.when(tile < tiles - 1)
    def _():
        tail_copy.wait_send()


def fused(tiles, latent, intersections, gain_one, shift_one, weight_one, gain_two, shift_two, weight_two, bias):
    _, frames, height, own_width, channels = latent.shape
    width, half, rows = 4 * own_width, channels // 2, height // 2
    early = frames // 4
    middle = (frames - early) // 2
    chunks_one = (early, middle, frames - early - middle)
    rest = frames - OVMAX
    chunks_two = ((rest, OVMAX), (0, rest // 2), (rest // 2, rest - rest // 2))
    shard = weight_one.shape[3]
    anywhere = pl.BlockSpec(memory_space=pl.ANY)
    spot = frames * rows
    sems = pltpu.SemaphoreType.DMA
    own_block = latent.shape[1:]
    return pl.pallas_call(
        functools.partial(block_kernel, tiles, chunks_one, chunks_two),
        out_shape=pltpu.VMEM(own_block, jnp.bfloat16),
        in_specs=[pl.BlockSpec(memory_space=pltpu.HBM)] * 9,
        out_specs=pl.BlockSpec(memory_space=pltpu.VMEM),
        scratch_shapes=[
            pltpu.SMEM((1,), jnp.int32),
            pltpu.VMEM(own_block, jnp.bfloat16),
            pltpu.VMEM((5, 1, channels), jnp.float32),
            pltpu.VMEM((27, half, channels), jnp.bfloat16),
            pltpu.VMEM((27, half, channels), jnp.bfloat16),
            pltpu.VMEM((4, frames, height, own_width, half), jnp.bfloat16),
            pltpu.VMEM((frames, height, width, half), jnp.float32),
            pltpu.VMEM((frames + 2, height + 2, width, 3 * half), jnp.bfloat16),
            pltpu.VMEM((frames + 2, height * 2 * own_width, 9 * half), jnp.bfloat16),
            pltpu.VMEM((spot * width, half), jnp.bfloat16),
            pltpu.VMEM((spot * width, half), jnp.bfloat16),
            pltpu.VMEM((spot * width, half), jnp.float32),
            pltpu.VMEM((frames, height, width, half), jnp.bfloat16),
            pltpu.VMEM(own_block, jnp.bfloat16),
            pltpu.VMEM(own_block, jnp.bfloat16),
            pltpu.VMEM(own_block, jnp.float32),
            pltpu.VMEM((OVMAX,) + own_block[1:], jnp.bfloat16),
            sems((7,)),
            sems((2,)),
            sems((2,)),
            sems((2,)),
            sems((3,)),
            sems((3,)),
            sems((len(chunks_one),)),
            sems((len(chunks_one),)),
            sems((len(chunks_one),)),
            sems((len(chunks_one),)),
            sems((len(chunks_two),)),
            sems((len(chunks_two),)),
            sems,
            sems,
        ],
        compiler_params=pltpu.CompilerParams(
            collective_id=0, has_side_effects=True, vmem_limit_bytes=60 * 2**20
        ),
    )(
        intersections,
        latent[0],
        gain_one[None],
        shift_one[None],
        gain_two[None],
        shift_two[None],
        bias[None],
        weight_one.reshape(27, shard, channels),
        weight_two.reshape(27, shard, channels),
    )[None]


def program(tiles, cols, *args):
    _, frames, height, own_width, channels = args[0].shape
    fits = (
        cols == 4
        and channels == 2 * LANES
        and own_width == 4
        and height % 2 == 0
        and frames >= 2 * OVMAX
    )
    return fused(tiles, *args) if fits else shards(*args)


def solution(mesh):
    in_specs = (
        P("tile", None, None, "col", None),
        P("tile"),
        P(),
        P(),
        P(None, None, None, "col", None),
        P(),
        P(),
        P(None, None, None, "col", None),
        P(),
    )
    out_specs = P("tile", None, None, "col", None)
    return jax.shard_map(
        functools.partial(program, mesh.shape["tile"], mesh.shape["col"]), mesh=mesh, in_specs=in_specs, out_specs=out_specs, check_vma=False)
```

```python
import functools

import jax
import jax.numpy as jnp
from jax import lax
from jax.experimental import pallas as pl
from jax.experimental.pallas import tpu as pltpu
from jax.sharding import PartitionSpec as P

GROUPS = 32
OVMAX = 4


epsilon = 1e-06


def extended_2(array, sides, width):
    for axis, dim in sides:
        size, length = (lax.axis_size(axis), array.shape[dim])
        up = [(i, (i + 1) % size) for i in range(size - 1)]
        down = [(j, i) for i, j in up]
        last = lax.slice_in_dim(array, length - width, length, axis=dim)
        first = lax.slice_in_dim(array, 0, width, axis=dim)
        before = lax.ppermute(last, axis, up)
        after = lax.ppermute(first, axis, down)
        array = jnp.concatenate([before, array, after], axis=dim)
    return array


def shifted(block, axis, distance):
    devices = range(lax.axis_size(axis))
    route = [(i - distance, i) for i in devices if i - distance in devices]
    return lax.ppermute(block, axis, route)


def conv_taps(padded, kernel):
    frames = padded.shape[0]
    height = padded.shape[1]
    out_width = padded.shape[2] - 2
    channels = padded.shape[3]
    outputs = kernel.shape[4]
    padded = jnp.pad(padded, ((2, 0), (1, 1), (0, 0), (0, 0)))
    running = jnp.zeros((frames * height * out_width, outputs), jnp.float32)
    for tap_t in range(3):
        for tap_h in range(3):
            for tap_w in range(3):
                window = padded[
                    tap_t : tap_t + frames, tap_h : tap_h + height, tap_w : tap_w + out_width
                ]
                running = running + jnp.dot(
                    window.reshape(-1, channels),
                    kernel[tap_t, tap_h, tap_w],
                    preferred_element_type=jnp.float32,
                )
    return running.reshape(frames, height, out_width, outputs)


def conv_layer(padded, weight_shard):
    return conv_taps(padded, lax.all_gather(weight_shard, "col", axis=3, tiled=True))


def group_total(values, per_group):
    return jnp.sum(values, axis=(0, 1, 2)).reshape(GROUPS, per_group).sum(axis=1)


def norm_silu(values, inner, gain, shift):
    channels = values.shape[3]
    per_group = channels // GROUPS
    members = inner.shape[0] * inner.shape[1] * inner.shape[2] * lax.axis_size("col") * per_group
    chan_sums = group_total(inner, per_group)
    group_mean = lax.psum(chan_sums, "col") / members
    centred = inner - jnp.repeat(group_mean, per_group)
    spread = lax.psum(group_total(centred * centred, per_group), "col") / members
    inv_std = lax.rsqrt(spread + epsilon)
    normed = (values - jnp.repeat(group_mean, per_group)) * jnp.repeat(
        inv_std, per_group
    ) * gain + shift
    return jax.nn.silu(normed).astype(jnp.bfloat16)


def shards(
    latent,
    intersections,
    norm_gain_one,
    norm_shift_one,
    weight_one,
    norm_gain_two,
    norm_shift_two,
    weight_two,
    conv_bias,
):
    source = latent[0]
    latent_full = source.astype(jnp.float32)
    act_one = norm_silu(latent_full, latent_full, norm_gain_one, norm_shift_one)
    margin = extended_2(act_one, (("col", 2),), 2)
    hidden = conv_layer(margin, weight_shard=weight_one).astype(jnp.bfloat16)
    hidden_full = hidden.astype(jnp.float32)
    act_two = norm_silu(hidden_full, hidden_full[:, :, 1:-1], norm_gain_two, norm_shift_two)
    own_width = source.shape[2]
    position = lax.axis_index("col") * own_width - 1 + jnp.arange(own_width + 2, dtype=jnp.int32)
    inside = (position >= 0) & (position < own_width * lax.axis_size("col"))
    act_two = jnp.where(inside[None, None, :, None], act_two, jnp.zeros_like(act_two))
    branch = conv_layer(act_two, weight_shard=weight_two)
    decoded = (latent_full + (branch + conv_bias)).astype(jnp.bfloat16)
    frames = decoded.shape[0]
    received = shifted(decoded[frames - OVMAX :], "tile", 1)
    shared = intersections[0]
    extended = jnp.concatenate([received, jnp.zeros_like(received)], axis=0)
    aligned = lax.dynamic_slice_in_dim(extended, OVMAX - shared, OVMAX, 0)
    position_t = jnp.arange(OVMAX, dtype=jnp.int32)
    own_share = ((position_t + 1).astype(jnp.float32) / (shared + 1).astype(jnp.float32))[
        :, None, None, None
    ]
    head = decoded[:OVMAX].astype(jnp.float32)
    active = (position_t < shared)[:, None, None, None]
    mixed = jnp.where(
        active, own_share * head + (1.0 - own_share) * aligned.astype(jnp.float32), head
    )
    blended = jnp.concatenate([mixed.astype(jnp.bfloat16), decoded[OVMAX:]], axis=0)
    return blended[None]


MESH = pl.DeviceIdType.MESH
LANES = 128


def group_sum(row, per_group):
    lane = lax.broadcasted_iota(jnp.int32, row.shape, 1)
    width = row.shape[1]
    step = 1
    while step < per_group:
        up = pltpu.roll(row, width - step, 1)
        down = pltpu.roll(row, step, 1)
        row = row + jnp.where((lane & step) == 0, up, down)
        step *= 2
    return row


def norm_of(frames, lines, store, gain, shift, per_group):
    height, width, _ = lines(0).shape
    members = frames * height * width * per_group

    def total(f):
        acc = jnp.zeros((8, LANES), jnp.float32)
        for t in range(frames):
            acc = acc + f(lines(t)).reshape(-1, 8, LANES).sum(axis=0)
        row = jnp.broadcast_to(acc.sum(axis=0, keepdims=True), (8, LANES))
        return group_sum(row, per_group)[0:1] / members

    mean = total(lambda v: v)

    def square(v):
        d = v - mean[None]
        return d * d

    scale = lax.rsqrt(total(square) + epsilon)
    where = lax.broadcasted_iota(jnp.int32, (height, width, LANES), 1)
    factor = scale * gain

    def normalise(times):
        for t in times:
            v = (lines(t) - mean[None]) * factor[None] + shift[None]
            b = 0.5 * v
            a = b + b * jnp.tanh(b)
            left = jnp.where(where == 0, 0.0, pltpu.roll(a, 1, 1))
            right = jnp.where(where == width - 1, 0.0, pltpu.roll(a, width - 1, 1))
            store(t, (left, a, right))

    return normalise


def conv_part(taps, weight, first, count, row, rows):
    width, depth = taps.shape[2], taps.shape[3]
    pieces = []
    for dt in range(3):
        for dh in range(3):
            window = taps[pl.ds(first + dt, count), pl.ds(row + dh, rows)]
            pieces.append(window.reshape(count * rows * width, depth))
    lhs = jnp.concatenate(pieces, axis=1)
    rhs = weight[...].reshape(9 * depth, weight.shape[2])
    return jnp.dot(lhs, rhs, preferred_element_type=jnp.float32)


def conv_packed(taps, weight, first, count):
    rows, depth = taps.shape[1], taps.shape[2]
    pieces = [taps[pl.ds(first + dt, count)].reshape(count * rows, depth) for dt in range(3)]
    lhs = jnp.concatenate(pieces, axis=1)
    rhs = weight[...].reshape(3 * depth, weight.shape[2])
    return jnp.dot(lhs, rhs, preferred_element_type=jnp.float32)


def block_kernel(
    tiles,
    chunks_one,
    chunks_two,
    inter_hbm,
    lat_hbm,
    gain_one_hbm,
    shift_one_hbm,
    gain_two_hbm,
    shift_two_hbm,
    bias_hbm,
    w_one,
    w_two,
    out,
    inter,
    lat,
    small,
    wb_one,
    wb_two,
    got,
    full,
    taps,
    packed,
    part_out,
    part_in,
    keep_one,
    hid,
    mix_out,
    mix_in,
    keep_two,
    tail_in,
    in_sem,
    w_local,
    w_send,
    w_recv,
    l_send,
    l_recv,
    p_send,
    p_recv,
    h_send,
    h_recv,
    m_send,
    m_recv,
    t_send,
    t_recv,
):
    tile = lax.axis_index("tile")
    me = lax.axis_index("col")
    chip = me // 2
    core = me % 2
    partner = chip * 2 + (1 - core)
    twin = (1 - chip) * 2 + core
    frames, height, own_width, channels = lat.shape
    shard = channels // 4
    half = channels // 2
    rows = height // 2
    width = 4 * own_width

    def remote(src, dst, send, recv, col):
        return pltpu.make_async_remote_copy(
            src_ref=src,
            dst_ref=dst,
            send_sem=send,
            recv_sem=recv,
            device_id={"tile": tile, "col": col},
            device_id_type=MESH,
        )

    barrier = pltpu.get_barrier_semaphore()
    for col in (partner, twin):
        pl.semaphore_signal(
            barrier, inc=1, device_id={"tile": tile, "col": col}, device_id_type=MESH
        )

    @pl.when(tile > 0)
    def _():
        pl.semaphore_signal(
            barrier, inc=1, device_id={"tile": tile - 1, "col": me}, device_id_type=MESH
        )

    lat_copy = pltpu.make_async_copy(lat_hbm, lat, in_sem.at[0])
    lat_copy.start()
    vectors = (gain_one_hbm, shift_one_hbm, gain_two_hbm, shift_two_hbm, bias_hbm)
    loads = [pltpu.make_async_copy(inter_hbm, inter, in_sem.at[1])]
    for k, vector in enumerate(vectors):
        loads.append(pltpu.make_async_copy(vector, small.at[k], in_sem.at[2 + k]))
    for copy in loads:
        copy.start()
    mine_rows = pl.ds(pl.multiple_of(core * shard, shard), shard)
    w_copies = []
    for k, (w, wb) in enumerate(((w_one, wb_one), (w_two, wb_two))):
        copy = pltpu.make_async_copy(w, wb.at[:, mine_rows, :], w_local.at[k])
        copy.start()
        w_copies.append(copy)

    first_chip = chip == 0
    first_core = core == 0
    here = pl.ds(pl.multiple_of(chip * half, half), half)
    there = pl.ds(pl.multiple_of((1 - chip) * half, half), half)
    to_twin = remote(lat.at[:, :, :, there], got.at[me], l_send.at[0], l_recv.at[0], twin)
    to_partner = remote(lat.at[:, :, :, here], got.at[me], l_send.at[1], l_recv.at[1], partner)
    forward = remote(got.at[twin], got.at[twin], l_send.at[2], l_recv.at[2], partner)
    w_sends = [
        remote(w, wb.at[:, mine_rows, :], w_send.at[k], w_recv.at[k], partner)
        for k, (w, wb) in enumerate(((w_one, wb_one), (w_two, wb_two)))
    ]

    lat_copy.wait()
    pl.semaphore_wait(barrier, 2 + jnp.where(tile < tiles - 1, 1, 0))
    to_twin.start()
    to_partner.start()
    w_sends[0].start()

    got[me] = jnp.where(first_chip, lat[:, :, :, :half], lat[:, :, :, half:])
    taps[0:2] = jnp.zeros((2,) + taps.shape[1:], taps.dtype)
    edge = jnp.zeros((frames,) + taps.shape[2:], taps.dtype)
    taps[2:, 0] = edge
    taps[2:, height + 1] = edge
    packed[0:2] = jnp.zeros((2,) + packed.shape[1:], packed.dtype)

    for copy in loads:
        copy.wait()

    def chosen(k):
        return jnp.where(first_chip, small[k][:, :half], small[k][:, half:])

    def store_taps(t, three):
        for k, value in enumerate(three):
            place = (t + 2, pl.ds(1, height), slice(None), pl.ds(k * LANES, LANES))
            taps[place] = value.astype(jnp.bfloat16)

    cols = 2 * own_width
    sub = lax.broadcasted_iota(jnp.int32, (height, cols, LANES), 1)

    def store_packed(t, three):
        zero = jnp.zeros((1, cols, LANES), jnp.float32)
        for k, value in enumerate(three):
            lo, hi = value[:, :cols], value[:, cols:]
            low = jnp.where(first_core, lo, pltpu.roll(lo, own_width, 1))
            high = jnp.where(first_core, pltpu.roll(hi, own_width, 1), hi)
            line = jnp.where(sub < own_width, low, high)
            moved = (
                jnp.concatenate([zero, line[:-1]], axis=0),
                line,
                jnp.concatenate([line[1:], zero], axis=0),
            )
            for dh, lines in enumerate(moved):
                value = lines.reshape(height * cols, LANES).astype(jnp.bfloat16)
                packed[t + 2, :, pl.ds((dh * 3 + k) * LANES, LANES)] = value

    def widen(side):
        for k in range(2):
            span = slice(k * own_width, (k + 1) * own_width)
            full[:, :, side, span, :] = got[2 * side + k].astype(jnp.float32)

    to_partner.wait_recv()
    widen(chip)
    to_twin.wait_recv()
    forward.start()
    w_sends[1].start()
    forward.wait_recv()
    widen(1 - chip)

    per_group = channels // GROUPS
    normalise = norm_of(frames, lambda t: full[t].reshape(height, width, half), store_taps, chosen(0), chosen(1), per_group)

    row = core * rows
    sends = []
    start = 0
    for k, count in enumerate(chunks_one):
        normalise(range(start, start + count))
        if k == 0:
            w_copies[0].wait()
            w_sends[0].wait()
        acc = conv_part(taps, wb_one, start, count, row, rows)
        lo, hi = acc[:, :half], acc[:, half:]
        span = pl.ds(start * rows * width, count * rows * width)
        part_out[span] = jnp.where(first_chip, hi, lo).astype(jnp.bfloat16)
        copy = remote(part_out.at[span], part_in.at[span], p_send.at[k], p_recv.at[k], twin)
        copy.start()
        keep_one[span] = jnp.where(first_chip, lo, hi)
        sends.append((copy, span, start, count))
        start += count
    back = []
    for k, (copy, span, first, count) in enumerate(sends):
        copy.wait_recv()
        value = keep_one[span] + part_in[span].astype(jnp.float32)
        place = (pl.ds(first, count), pl.ds(row, rows))
        hid[place] = value.astype(jnp.bfloat16).reshape(count, rows, width, half)
        copy = remote(hid.at[place], hid.at[place], h_send.at[k], h_recv.at[k], partner)
        copy.start()
        back.append(copy)
    for copy in back:
        copy.wait_recv()

    normalise = norm_of(
        frames,
        lambda t: hid[t].astype(jnp.float32),
        store_packed,
        chosen(2),
        chosen(3),
        per_group,
    )

    done = set()
    offset = small[4][None, None]
    sends_two = []
    for k, (first, count) in enumerate(chunks_two):
        needed = [t for t in range(max(first - 2, 0), first + count) if t not in done]
        normalise(needed)
        done.update(needed)
        if k == 0:
            w_copies[1].wait()
            w_sends[1].wait()
        acc = conv_packed(packed, wb_two, first, count)
        acc = acc.reshape(count, height, cols, channels)
        lo, hi = acc[:, :, :own_width], acc[:, :, own_width:]
        times = pl.ds(first, count)
        mix_out[times] = jnp.where(first_chip, hi, lo).astype(jnp.bfloat16)
        copy = remote(mix_out.at[times], mix_in.at[times], m_send.at[k], m_recv.at[k], twin)
        copy.start()
        own = jnp.where(first_chip, lo, hi)
        keep_two[times] = lat[times].astype(jnp.float32) + (own + offset)
        sends_two.append((copy, times))

    overlap = OVMAX
    next_tile = jnp.minimum(tile + 1, tiles - 1)
    tail_copy = pltpu.make_async_remote_copy(
        src_ref=out.at[pl.ds(frames - overlap, overlap)],
        dst_ref=tail_in,
        send_sem=t_send,
        recv_sem=t_recv,
        device_id={"tile": next_tile, "col": me},
        device_id_type=MESH,
    )
    for k, (copy, times) in enumerate(sends_two):
        copy.wait_recv()
        value = keep_two[times] + mix_in[times].astype(jnp.float32)
        out[times] = value.astype(jnp.bfloat16)
        if k == 0:

            @pl.when(tile < tiles - 1)
            def _():
                tail_copy.start()

    @pl.when(tile > 0)
    def _():
        tail_copy.wait_recv()

    @pl.when(tile == 0)
    def _():
        tail_in[...] = jnp.zeros(tail_in.shape, tail_in.dtype)

    shared = inter[0]
    whole = jnp.full((height, own_width, channels), shared + 1, jnp.int32).astype(jnp.float32)
    for j in range(overlap):
        u = (j + 1) / whole
        before = tail_in[jnp.clip(overlap - shared + j, 0, overlap - 1)].astype(jnp.float32)
        value = out[j].astype(jnp.float32)
        mixed = jnp.where(j < shared, u * value + (1.0 - u) * before, value)
        out[j] = mixed.astype(jnp.bfloat16)

    to_twin.wait_send()
    to_partner.wait_send()
    forward.wait_send()
    for copy, *_ in sends + sends_two:
        copy.wait_send()
    for copy in back:
        copy.wait_send()

    @pl.when(tile < tiles - 1)
    def _():
        tail_copy.wait_send()


def fused(tiles, latent, intersections, gain_one, shift_one, weight_one, gain_two, shift_two, weight_two, bias):
    _, frames, height, own_width, channels = latent.shape
    width, half, rows = 4 * own_width, channels // 2, height // 2
    early = frames // 4
    middle = (frames - early) // 2
    chunks_one = (early, middle, frames - early - middle)
    rest = frames - OVMAX
    chunks_two = ((rest, OVMAX), (0, rest // 2), (rest // 2, rest - rest // 2))
    shard = weight_one.shape[3]
    anywhere = pl.BlockSpec(memory_space=pl.ANY)
    spot = frames * rows
    sems = pltpu.SemaphoreType.DMA
    own_block = latent.shape[1:]
    return pl.pallas_call(
        functools.partial(block_kernel, tiles, chunks_one, chunks_two),
        out_shape=pltpu.VMEM(own_block, jnp.bfloat16),
        in_specs=[pl.BlockSpec(memory_space=pltpu.HBM)] * 9,
        out_specs=pl.BlockSpec(memory_space=pltpu.VMEM),
        scratch_shapes=[
            pltpu.SMEM((1,), jnp.int32),
            pltpu.VMEM(own_block, jnp.bfloat16),
            pltpu.VMEM((5, 1, channels), jnp.float32),
            pltpu.VMEM((27, half, channels), jnp.bfloat16),
            pltpu.VMEM((27, half, channels), jnp.bfloat16),
            pltpu.VMEM((4, frames, height, own_width, half), jnp.bfloat16),
            pltpu.VMEM((frames, height, 2, width // 2, half), jnp.float32),
            pltpu.VMEM((frames + 2, height + 2, width, 3 * half), jnp.bfloat16),
            pltpu.VMEM((frames + 2, height * 2 * own_width, 9 * half), jnp.bfloat16),
            pltpu.VMEM((spot * width, half), jnp.bfloat16),
            pltpu.VMEM((spot * width, half), jnp.bfloat16),
            pltpu.VMEM((spot * width, half), jnp.float32),
            pltpu.VMEM((frames, height, width, half), jnp.bfloat16),
            pltpu.VMEM(own_block, jnp.bfloat16),
            pltpu.VMEM(own_block, jnp.bfloat16),
            pltpu.VMEM(own_block, jnp.float32),
            pltpu.VMEM((OVMAX,) + own_block[1:], jnp.bfloat16),
            sems((7,)),
            sems((2,)),
            sems((2,)),
            sems((2,)),
            sems((3,)),
            sems((3,)),
            sems((len(chunks_one),)),
            sems((len(chunks_one),)),
            sems((len(chunks_one),)),
            sems((len(chunks_one),)),
            sems((len(chunks_two),)),
            sems((len(chunks_two),)),
            sems,
            sems,
        ],
        compiler_params=pltpu.CompilerParams(
            collective_id=0, has_side_effects=True, vmem_limit_bytes=60 * 2**20
        ),
    )(
        intersections,
        latent[0],
        gain_one[None],
        shift_one[None],
        gain_two[None],
        shift_two[None],
        bias[None],
        weight_one.reshape(27, shard, channels),
        weight_two.reshape(27, shard, channels),
    )[None]


def program(tiles, cols, *args):
    _, frames, height, own_width, channels = args[0].shape
    fits = (
        cols == 4
        and channels == 2 * LANES
        and own_width == 4
        and height % 2 == 0
        and frames >= 2 * OVMAX
    )
    return fused(tiles, *args) if fits else shards(*args)


def solution(mesh):
    in_specs = (
        P("tile", None, None, "col", None),
        P("tile"),
        P(),
        P(),
        P(None, None, None, "col", None),
        P(),
        P(),
        P(None, None, None, "col", None),
        P(),
    )
    out_specs = P("tile", None, None, "col", None)
    return jax.shard_map(
        functools.partial(program, mesh.shape["tile"], mesh.shape["col"]), mesh=mesh, in_specs=in_specs, out_specs=out_specs, check_vma=False)
```
